32 devices in a mesh: groups: 2 (over x), ha: 16 (over z, y, core).
Axes of the slice: x: 2, y: 2, z: 4, core: 2. Of those that a mesh axis runs over, the one named last changes fastest.
Arguments:
- video: bfloat16 [8, 64, 256, 128], P('groups', 'ha'), parts along dimension 0, may hold values from -90 to 90
- cache_video: bfloat16 [4, 64, 256, 128], P('groups', 'ha'), parts along dimension 0, may hold values from -90 to 90
- cache_hidden: bfloat16 [4, 32, 128, 256], P('groups', 'ha'), parts along dimension 0, may hold values from -0.25 to 2
- kernel_down: bfloat16 [3, 3, 3, 128, 256], replicated, may hold values from -0.05103104 to 0.05103104
- gain_down: float32 [256], replicated, may hold values from 0.1 to 1.9
- shift_down: float32 [256], replicated, may hold values from -3 to 3
- kernel_mix: bfloat16 [3, 3, 3, 256, 256], replicated, may hold values from -0.03608439 to 0.03608439
- gain_mix: float32 [256], replicated, may hold values from 0.1 to 1.9
- shift_mix: float32 [256], replicated, may hold values from -3 to 3
Outputs:
- encoded: bfloat16 [8, 32, 128, 256], P('groups', 'ha'), parts along dimension 0
- next_cache: bfloat16 [4, 32, 128, 256], P('groups', 'ha'), parts along dimension 0
The draws below stay inside these ranges and needn't reach their ends.
There are 2 independent parts, one for each index of `groups`. The reference program is written for one: setup_inputs(seed, part) draws one part's arguments, and reference() takes and returns one part's arrays. A program takes and returns all parts, laid end to end along the dimension named above; an argument that names none is the same for every part. Nothing has to cross between parts.
All inputs are finite; a program needn't handle non-finite values.
Results may differ from the reference program's by a relative error of at most 0.0032.
Values may be sent and summed in bfloat16 or wider, within the bound.
A program may use at most 64 MiB of HBM per device.

```python
import math
import jax
import jax.numpy as jnp
from jax import lax

C_IN = 128
C_OUT = 256
GROUPS = 32
FRAMES = 4
WIDTH = 256
HEIGHT = 64


def rough_noise(key, shape):
    return jnp.clip(jax.random.normal(key, shape, jnp.float32), -6.0, 6.0)


def scale_profiles(key):
    keys = jax.random.split(jax.random.fold_in(key, 7), 2)
    rising = jnp.exp(math.log(3.0) * jnp.arange(HEIGHT, dtype=jnp.float32) / HEIGHT)
    rowwise = rising * jnp.exp(jax.random.uniform(keys[0], (HEIGHT,), jnp.float32, 0.0, math.log(3.3)))
    columns = jnp.exp(jax.random.uniform(keys[1], (WIDTH,), jnp.float32, 0.0, math.log(10.0)))
    return (rowwise, columns)


def frames_field(key, own_key, frames):
    shared = rough_noise(jax.random.fold_in(key, 5), (1, HEIGHT, WIDTH, C_IN))
    own = rough_noise(own_key, (frames, HEIGHT, WIDTH, C_IN))
    base = 0.9 * shared + 0.44 * own
    rowwise, columns = scale_profiles(key)
    return 0.1 * base * rowwise[None, :, None, None] * columns[None, None, :, None]


def tap_kernel(key, fan_rows, fan_cols):
    keys = jax.random.split(key, 2)
    share = 0.25
    common = jax.random.normal(keys[0], (1, 1, 1, fan_rows, fan_cols), jnp.float32)
    taps = jax.random.normal(keys[1], (3, 3, 3, fan_rows, fan_cols), jnp.float32)
    limit = 0.99 * 3.0 / math.sqrt(27 * fan_rows)
    values = (math.sqrt(share) * common + math.sqrt(1.0 - share) * taps) / math.sqrt(27 * fan_rows)
    return jnp.clip(values, -limit, limit)


def draw_video(key, part):
    return frames_field(key, jax.random.fold_in(key, 11), FRAMES).astype(jnp.bfloat16)


def draw_cache_video(key, part):
    return frames_field(key, jax.random.fold_in(key, 23), 2).astype(jnp.bfloat16)


def draw_kernel_down(key, part):
    return tap_kernel(jax.random.fold_in(key, 31), C_IN, C_OUT).astype(jnp.bfloat16)


def draw_kernel_mix(key, part):
    return tap_kernel(jax.random.fold_in(key, 37), C_OUT, C_OUT).astype(jnp.bfloat16)


def block_levels(rng, extent, cuts, smallest, high):
    loudness = 1.0
    for dim, parts in cuts:
        heights = jax.random.uniform(jax.random.fold_in(jax.random.fold_in(rng, 6), dim), (parts,), jnp.float32, smallest / len(cuts), high / len(cuts))
        loudness = loudness * jnp.repeat(jnp.exp(heights), extent[dim] // parts).reshape((-1,) + (1,) * (len(extent) - 1 - dim))
    return loudness


def gaussian(rng, extent, scale, most, held_as=jnp.bfloat16):
    values = scale * jax.random.normal(rng, extent, jnp.float32)
    return jnp.clip(values, min=-most, max=most).astype(held_as)


def setup_inputs(seed: int = 0, part: int = 0) -> dict:
    splits = jax.random.split(jax.random.key(seed), 10)
    part_keys = jax.random.split(jax.random.fold_in(splits[9], part), 10)
    return {
        "video": draw_video(jax.random.fold_in(jax.random.fold_in(splits[9], part), 71), part),
        "cache_video": draw_cache_video(jax.random.fold_in(jax.random.fold_in(splits[9], part), 71), part),
        "cache_hidden": jnp.clip(-0.25 + 2.25 * jax.random.uniform(part_keys[2], (2, HEIGHT // 2, WIDTH // 2, C_OUT), jnp.float32) ** block_levels(part_keys[2], (2, HEIGHT // 2, WIDTH // 2, C_OUT), ((1, 16),), -0.2, 0.2), -0.25, 2.0).astype(jnp.bfloat16),
        "kernel_down": draw_kernel_down(jax.random.fold_in(splits[9], 71), part),
        "gain_down": jnp.clip(1.0 + 0.18 * jax.random.normal(splits[4], (C_OUT,), jnp.float32), 0.1, 1.9),
        "shift_down": gaussian(splits[5], (C_OUT,), 0.5, 3.0, jnp.float32),
        "kernel_mix": draw_kernel_mix(jax.random.fold_in(splits[9], 71), part),
        "gain_mix": jnp.clip(1.0 + 0.18 * jax.random.normal(splits[7], (C_OUT,), jnp.float32), 0.1, 1.9),
        "shift_mix": gaussian(splits[8], (C_OUT,), 0.5, 3.0, jnp.float32),
    }


def convolve(stack, kernel, strides):
    result = lax.conv_general_dilated(stack[None], kernel, strides, 'VALID', dimension_numbers=('NDHWC', 'DHWIO', 'NDHWC'), preferred_element_type=jnp.float32)
    return result[0]

def normalize(values, scales, offsets):
    per_group = values.shape[-1] // GROUPS
    members = values.shape[0] * values.shape[1] * values.shape[2] * per_group
    totals = lax.optimization_barrier(jnp.sum(values, axis=(0, 1, 2))).reshape(GROUPS, per_group).sum(1)
    center = jnp.repeat(totals / members, per_group)
    deviate = values - center
    squares = lax.optimization_barrier(jnp.sum(deviate * deviate, axis=(0, 1, 2))).reshape(GROUPS, per_group).sum(1)
    spread = jnp.repeat(squares / members, per_group)
    normed = deviate * lax.rsqrt(spread + 1e-06) * scales + offsets
    return jax.nn.silu(normed).astype(jnp.bfloat16)

def reference(video, cache_video, cache_hidden, kernel_down, gain_down, shift_down, kernel_mix, gain_mix, shift_mix):
    stacked = jnp.concatenate([cache_video, video], axis=0)
    stacked = jnp.pad(stacked, ((0, 0), (0, 1), (0, 1), (0, 0)))
    first = convolve(stacked, kernel_down, (1, 2, 2))
    hidden = normalize(first, gain_down, shift_down)
    padded = jnp.concatenate([cache_hidden, hidden], axis=0)
    padded = jnp.pad(padded, ((0, 0), (1, 1), (1, 1), (0, 0)))
    second = convolve(padded, kernel_mix, (1, 1, 1))
    encoded = normalize(second, gain_mix, shift_mix)
    return (encoded, hidden[FRAMES - 2:])
```

```python
import functools

import jax
import jax.numpy as jnp
from jax import lax
from jax.experimental import pallas as pl
from jax.experimental.pallas import tpu as pltpu
from jax.sharding import PartitionSpec as P

GROUPS = 32
MESH = pl.DeviceIdType.MESH
F32 = jnp.float32
BF16 = jnp.bfloat16


def kernel(
    n,
    video,
    cache_video,
    cache_hidden,
    w_down,
    gain_down,
    shift_down,
    w_mix,
    gain_mix,
    shift_mix,
    encoded,
    next_cache,
    vid,
    rim,
    raw,
    x1,
    w1,
    w2,
    x2,
    acc1,
    acc2,
    right,
    left,
    stats,
    enc,
    load_sem,
    rim_send,
    rim_recv,
    hid_send,
    hid_recv,
    stat_send,
    stat_recv,
    out_sem,
):
    frames, rows, width, c_in = video.shape
    past = cache_video.shape[0]
    total = frames + past
    out_rows, cols, c_out = cache_hidden.shape[1:]
    m = frames * cols
    me = lax.axis_index("ha")
    has_up = me > 0
    has_down = me < n - 1

    barrier = pltpu.get_barrier_semaphore()

    @pl.loop(1, n)
    def _(k):
        pl.semaphore_signal(barrier, inc=1, device_id={"ha": lax.rem(me + k, n)}, device_id_type=MESH)

    loads = []
    for t in range(total):
        src = cache_video.at[t] if t < past else video.at[t - past]
        loads.append((src, vid.at[t]))
    for a in range(3):
        loads.append((w_down.at[pl.ds(3 * a, 3)], w1.at[pl.ds(3 * a, 3)]))
    for a in range(3):
        loads.append((w_mix.at[pl.ds(3 * a, 3)], w2.at[pl.ds(3 * a, 3)]))
    for t in range(past):
        for r in range(out_rows):
            loads.append((cache_hidden.at[t, r], x2.at[1 + r, pl.ds(t * cols, cols)]))
    copies = [pltpu.make_async_copy(s, d, load_sem.at[i]) for i, (s, d) in enumerate(loads)]
    for copy in copies:
        copy.start()

    right[:, :, pl.ds(cols, 8), :] = jnp.zeros(right.shape[:2] + (8, c_out), F32)
    left[:, :, pl.ds(0, 8), :] = jnp.zeros(left.shape[:2] + (8, c_out), F32)

    def rim_copy(t):
        src = cache_video.at[t, 0] if t < past else video.at[t - past, 0]
        return pltpu.make_async_remote_copy(
            src_ref=src, dst_ref=rim.at[t], send_sem=rim_send.at[t], recv_sem=rim_recv.at[t],
            device_id={"ha": me - 1}, device_id_type=MESH,
        )

    def hid_copy(up, t):
        span = pl.ds(t * cols, cols)
        if t < past:
            src = cache_hidden.at[t, 0 if up else out_rows - 1]
        else:
            src = x2.at[1 if up else out_rows, span]
        side = 0 if up else 1
        return pltpu.make_async_remote_copy(
            src_ref=src, dst_ref=x2.at[out_rows + 1 if up else 0, span],
            send_sem=hid_send.at[side, t], recv_sem=hid_recv.at[side, t],
            device_id={"ha": me - 1 if up else me + 1}, device_id_type=MESH,
        )

    pl.semaphore_wait(barrier, n - 1)

    @pl.when(has_up)
    def _():
        for t in range(total):
            rim_copy(t).start()
        for t in range(past):
            hid_copy(True, t).start()

    @pl.when(has_down)
    def _():
        for t in range(past):
            hid_copy(False, t).start()

    @pl.when(jnp.logical_not(has_up))
    def _():
        x2[0] = jnp.zeros(x2.shape[1:], BF16)

    @pl.when(jnp.logical_not(has_down))
    def _():
        x2[out_rows + 1] = jnp.zeros(x2.shape[1:], BF16)
        x1[rows] = jnp.zeros(x1.shape[1:], BF16)

    def split(src, slot, r, t):
        raw[slot] = src.astype(F32)
        x1[r, pl.ds(t * cols, cols), 0:c_in] = raw[slot, pl.ds(0, cols, stride=2), :].astype(BF16)
        x1[r, pl.ds(t * cols, cols), c_in:] = raw[slot, pl.ds(1, cols, stride=2), :].astype(BF16)

    for t in range(total):
        copies[t].wait()
        for r in range(rows):
            split(vid[t, r], r, r, t)
    for a in range(3):
        copies[total + a].wait()

    def taps(x, lanes, w, depth, pairs):
        lhs = jnp.concatenate([x[r, pl.ds(a * cols, m), lanes] for a, r, b in pairs], axis=1)
        rhs = jnp.concatenate([w[3 * a + b, depth, :] for a, r, b in pairs], axis=0)
        return jnp.dot(lhs, rhs, preferred_element_type=F32)

    both, even = slice(0, 2 * c_in), slice(0, c_in)
    near, far = slice(0, 2 * c_in), slice(2 * c_in, 3 * c_in)

    def as_frames(v):
        return v.reshape(frames, cols, c_out)

    for i in range(out_rows):
        pairs = [(a, 2 * i + b, b) for b in range(3) if 2 * i + b < rows for a in range(3)]
        acc1[i] = taps(x1, both, w1, near, pairs)
        right[i, :, pl.ds(0, cols), :] = as_frames(taps(x1, even, w1, far, pairs))

    @pl.when(has_down)
    def _():
        for t in range(total):
            rim_copy(t).wait_recv()
            split(rim[t], t % rows, rows, t)

    pairs = [(a, rows, 2) for a in range(3)]
    last = out_rows - 1
    acc1[last] += taps(x1, both, w1, near, pairs)
    right[last, :, pl.ds(0, cols), :] += as_frames(taps(x1, even, w1, far, pairs))

    def sums(parts, s, q, v):
        v8 = v.reshape(cols // 8, 8, c_out)
        return s + jnp.sum(v8, axis=0), q + jnp.sum(v8 * v8, axis=0)

    def stat_copy(phase, owner, peer, k):
        return pltpu.make_async_remote_copy(
            src_ref=stats.at[phase, me], dst_ref=stats.at[phase, owner],
            send_sem=stat_send.at[phase, k], recv_sem=stat_recv.at[phase, owner],
            device_id={"ha": peer}, device_id_type=MESH,
        )

    def send_stats(phase, s, q):
        stats[phase, me] = jnp.concatenate(
            [jnp.sum(s, axis=0, keepdims=True), jnp.sum(q, axis=0, keepdims=True)], axis=0
        )

        @pl.loop(1, n)
        def _(k):
            stat_copy(phase, me, lax.rem(me + k, n), k).start()

    per_group = c_out // GROUPS
    members = float(frames * out_rows * n * cols * per_group)

    def wait_stats(phase):
        @pl.loop(1, n)
        def _(k):
            peer = lax.rem(me + k, n)
            stat_copy(phase, peer, peer, k).wait_recv()

        both_sums = jnp.sum(stats[phase], axis=0)
        lane = lax.broadcasted_iota(jnp.int32, (8, c_out), 1)

        def grouped(v):
            v = jnp.broadcast_to(v, (8, c_out))
            step = 1
            while step < per_group:
                below = pltpu.roll(v, step, 1)
                above = pltpu.roll(v, c_out - step, 1)
                v = v + jnp.where((lane & step) == 0, above, below)
                step *= 2
            return v[0:1]

        center = grouped(both_sums[0:1]) / members
        spread = jnp.maximum(grouped(both_sums[1:2]) / members - center * center, 0.0)
        return center, lax.rsqrt(spread + 1e-06)

    def activate(v, center, scale, shift):
        v = (v - center) * scale + shift
        return (v / (1.0 + jnp.exp(-v))).astype(BF16)

    s = q = jnp.zeros((8, c_out), F32)
    for i in range(out_rows):
        for t in range(frames):
            span = pl.ds(t * cols, cols)
            v = acc1[i, span, :] + right[i, t, pl.ds(1, cols), :]
            acc1[i, span, :] = v
            s, q = sums(None, s, q, v)
    send_stats(0, s, q)

    for i in range(total + 3, len(copies)):
        copies[i].wait()

    center, inverse = wait_stats(0)
    scale = inverse * gain_down[...]
    shift = shift_down[...]
    for t in range(frames):
        for i in range(out_rows):
            x2[1 + i, pl.ds((past + t) * cols, cols), :] = activate(
                acc1[i, pl.ds(t * cols, cols), :], center, scale, shift
            )

        @pl.when(has_up)
        def _():
            hid_copy(True, past + t).start()

        @pl.when(has_down)
        def _():
            hid_copy(False, past + t).start()

    outs = []
    for t in range(past):
        for r in range(out_rows):
            src = x2.at[1 + r, pl.ds((total - past + t) * cols, cols)]
            outs.append(pltpu.make_async_copy(src, next_cache.at[t, r], out_sem.at[len(outs)]))
            outs[-1].start()

    everything = slice(0, c_out)

    def mix(i, c, pairs):
        return taps(x2, everything, w2, pl.ds(c * c_out, c_out), pairs)

    for i in range(out_rows):
        pairs = [(a, i + b, b) for b in range(3) if 1 <= i + b <= out_rows for a in range(3)]
        left[i, :, pl.ds(8, cols), :] = as_frames(mix(i, 0, pairs))
        acc2[i] = mix(i, 1, pairs)
        right[i, :, pl.ds(0, cols), :] = as_frames(mix(i, 2, pairs))

    @pl.when(has_up)
    def _():
        for t in range(total):
            hid_copy(False, t).wait_recv()

    @pl.when(has_down)
    def _():
        for t in range(total):
            hid_copy(True, t).wait_recv()

    s = q = jnp.zeros((8, c_out), F32)
    for i in range(out_rows):
        pairs = [(a, i + b, b) for b in range(3) if not 1 <= i + b <= out_rows for a in range(3)]
        if pairs:
            left[i, :, pl.ds(8, cols), :] += as_frames(mix(i, 0, pairs))
            acc2[i] += mix(i, 1, pairs)
            right[i, :, pl.ds(0, cols), :] += as_frames(mix(i, 2, pairs))
        for t in range(frames):
            span = pl.ds(t * cols, cols)
            v = acc2[i, span, :] + left[i, t, pl.ds(7, cols), :] + right[i, t, pl.ds(1, cols), :]
            acc2[i, span, :] = v
            s, q = sums(None, s, q, v)
    send_stats(1, s, q)

    center, inverse = wait_stats(1)
    scale = inverse * gain_mix[...]
    shift = shift_mix[...]
    for t in range(frames):
        for i in range(out_rows):
            enc[t, i] = activate(acc2[i, pl.ds(t * cols, cols), :], center, scale, shift)
        outs.append(pltpu.make_async_copy(enc.at[t], encoded.at[t], out_sem.at[len(outs)]))
        outs[-1].start()

    @pl.when(has_up)
    def _():
        for t in range(total):
            rim_copy(t).wait_send()
            hid_copy(True, t).wait_send()

    @pl.when(has_down)
    def _():
        for t in range(total):
            hid_copy(False, t).wait_send()

    for phase in range(2):

        @pl.loop(1, n)
        def _(k):
            stat_copy(phase, me, lax.rem(me + k, n), k).wait_send()

    for copy in outs:
        copy.wait()


def local(n, video, cache_video, cache_hidden, kernel_down, gain_down, shift_down, kernel_mix, gain_mix, shift_mix):
    frames, rows, width, c_in = video.shape
    past, out_rows, cols, c_out = cache_hidden.shape
    total = frames + past
    hbm = pl.BlockSpec(memory_space=pl.ANY)
    vmem = pl.BlockSpec(memory_space=pltpu.VMEM)
    row = lambda v: v.reshape(1, c_out)
    return pl.pallas_call(
        functools.partial(kernel, n),
        out_shape=(
            jax.ShapeDtypeStruct((frames, out_rows, cols, c_out), BF16),
            jax.ShapeDtypeStruct((past, out_rows, cols, c_out), BF16),
        ),
        in_specs=[hbm, hbm, hbm, hbm, vmem, vmem, hbm, vmem, vmem],
        out_specs=(hbm, hbm),
        scratch_shapes=[
            pltpu.VMEM((total, rows, width, c_in), BF16),
            pltpu.VMEM((total, width, c_in), BF16),
            pltpu.VMEM((rows, width, c_in), F32),
            pltpu.VMEM((rows + 1, total * cols, 2 * c_in), BF16),
            pltpu.VMEM((9, 3 * c_in, c_out), BF16),
            pltpu.VMEM((9, 3 * c_out, c_out), BF16),
            pltpu.VMEM((out_rows + 2, total * cols, c_out), BF16),
            pltpu.VMEM((out_rows, frames * cols, c_out), F32),
            pltpu.VMEM((out_rows, frames * cols, c_out), F32),
            pltpu.VMEM((out_rows, frames, cols + 8, c_out), F32),
            pltpu.VMEM((out_rows, frames, cols + 8, c_out), F32),
            pltpu.VMEM((2, n, 2, c_out), F32),
            pltpu.VMEM((frames, out_rows, cols, c_out), BF16),
            pltpu.SemaphoreType.DMA((total + 6 + past * out_rows,)),
            pltpu.SemaphoreType.DMA((total,)),
            pltpu.SemaphoreType.DMA((total,)),
            pltpu.SemaphoreType.DMA((2, total)),
            pltpu.SemaphoreType.DMA((2, total)),
            pltpu.SemaphoreType.DMA((2, n)),
            pltpu.SemaphoreType.DMA((2, n)),
            pltpu.SemaphoreType.DMA((past * out_rows + frames,)),
        ],
        compiler_params=pltpu.CompilerParams(
            collective_id=0, has_side_effects=True, vmem_limit_bytes=48 * 1024 * 1024
        ),
    )(
        video,
        cache_video,
        cache_hidden,
        kernel_down.reshape(9, 3 * c_in, c_out),
        row(gain_down),
        row(shift_down),
        kernel_mix.reshape(9, 3 * c_out, c_out),
        row(gain_mix),
        row(shift_mix),
    )


def solution(mesh):
    split = P("groups", "ha", None, None)
    return jax.shard_map(
        functools.partial(local, mesh.shape["ha"]),
        mesh=mesh,
        in_specs=(split, split, split) + (P(),) * 6,
        out_specs=(split, split),
        check_vma=False,
    )
```

```python
import functools

import jax
import jax.numpy as jnp
from jax import lax
from jax.experimental import pallas as pl
from jax.experimental.pallas import tpu as pltpu
from jax.sharding import PartitionSpec as P

GROUPS = 32
MESH = pl.DeviceIdType.MESH
F32 = jnp.float32
BF16 = jnp.bfloat16


def kernel(
    n,
    video,
    cache_video,
    cache_hidden,
    w_down,
    gain_down,
    shift_down,
    w_mix,
    gain_mix,
    shift_mix,
    encoded,
    next_cache,
    vid,
    rim,
    raw,
    x1,
    w1,
    w2,
    x2,
    acc1,
    acc2,
    right,
    left,
    stats,
    params,
    load_sem,
    rim_send,
    rim_recv,
    hid_send,
    hid_recv,
    stat_send,
    stat_recv,
):
    frames, rows, width, c_in = video.shape
    past = cache_video.shape[0]
    total = frames + past
    out_rows, cols, c_out = cache_hidden.shape[1:]
    m = frames * cols
    me = lax.axis_index("ha")
    has_up = me > 0
    has_down = me < n - 1

    barrier = pltpu.get_barrier_semaphore()

    @pl.loop(1, n)
    def _(k):
        pl.semaphore_signal(barrier, inc=1, device_id={"ha": lax.rem(me + k, n)}, device_id_type=MESH)

    loads = []
    for t in range(total):
        src = cache_video.at[t] if t < past else video.at[t - past]
        loads.append((src, vid.at[t]))
    for a in range(3):
        loads.append((w_down.at[pl.ds(3 * a, 3)], w1.at[pl.ds(3 * a, 3)]))
    for a in range(3):
        loads.append((w_mix.at[pl.ds(3 * a, 3)], w2.at[pl.ds(3 * a, 3)]))
    for t in range(past):
        for r in range(out_rows):
            loads.append((cache_hidden.at[t, r], x2.at[1 + r, pl.ds(t * cols, cols)]))
    for i, param in enumerate((gain_down, shift_down, gain_mix, shift_mix)):
        loads.append((param, params.at[i]))
    copies = [pltpu.make_async_copy(s, d, load_sem.at[i]) for i, (s, d) in enumerate(loads)]
    for copy in copies:
        copy.start()

    right[:, :, pl.ds(cols, 8), :] = jnp.zeros(right.shape[:2] + (8, c_out), F32)
    left[:, :, pl.ds(0, 8), :] = jnp.zeros(left.shape[:2] + (8, c_out), F32)

    def rim_copy(t):
        src = cache_video.at[t, 0] if t < past else video.at[t - past, 0]
        return pltpu.make_async_remote_copy(
            src_ref=src, dst_ref=rim.at[t], send_sem=rim_send.at[t], recv_sem=rim_recv.at[t],
            device_id={"ha": me - 1}, device_id_type=MESH,
        )

    def hid_copy(up, t):
        span = pl.ds(t * cols, cols)
        if t < past:
            src = cache_hidden.at[t, 0 if up else out_rows - 1]
        else:
            src = x2.at[1 if up else out_rows, span]
        side = 0 if up else 1
        return pltpu.make_async_remote_copy(
            src_ref=src, dst_ref=x2.at[out_rows + 1 if up else 0, span],
            send_sem=hid_send.at[side, t], recv_sem=hid_recv.at[side, t],
            device_id={"ha": me - 1 if up else me + 1}, device_id_type=MESH,
        )

    pl.semaphore_wait(barrier, n - 1)

    @pl.when(has_up)
    def _():
        for t in range(total):
            rim_copy(t).start()
        for t in range(past):
            hid_copy(True, t).start()

    @pl.when(has_down)
    def _():
        for t in range(past):
            hid_copy(False, t).start()

    @pl.when(jnp.logical_not(has_up))
    def _():
        x2[0] = jnp.zeros(x2.shape[1:], BF16)

    @pl.when(jnp.logical_not(has_down))
    def _():
        x2[out_rows + 1] = jnp.zeros(x2.shape[1:], BF16)
        x1[rows] = jnp.zeros(x1.shape[1:], BF16)

    def split(src, slot, r, t):
        raw[slot] = src.astype(F32)
        x1[r, pl.ds(t * cols, cols), 0:c_in] = raw[slot, pl.ds(0, cols, stride=2), :].astype(BF16)
        x1[r, pl.ds(t * cols, cols), c_in:] = raw[slot, pl.ds(1, cols, stride=2), :].astype(BF16)

    for t in range(total):
        copies[t].wait()
        for r in range(rows):
            split(vid[t, r], r, r, t)
    for a in range(3):
        copies[total + a].wait()

    def taps(x, lanes, w, depth, pairs):
        lhs = jnp.concatenate([x[r, pl.ds(a * cols, m), lanes] for a, r, b in pairs], axis=1)
        rhs = jnp.concatenate([w[3 * a + b, depth, :] for a, r, b in pairs], axis=0)
        return jnp.dot(lhs, rhs, preferred_element_type=F32)

    both, even = slice(0, 2 * c_in), slice(0, c_in)
    near, far = slice(0, 2 * c_in), slice(2 * c_in, 3 * c_in)

    def as_frames(v):
        return v.reshape(frames, cols, c_out)

    for i in range(out_rows):
        pairs = [(a, 2 * i + b, b) for b in range(3) if 2 * i + b < rows for a in range(3)]
        acc1[i] = taps(x1, both, w1, near, pairs)
        right[i, :, pl.ds(0, cols), :] = as_frames(taps(x1, even, w1, far, pairs))

    @pl.when(has_down)
    def _():
        for t in range(total):
            rim_copy(t).wait_recv()
            split(rim[t], t % rows, rows, t)

    pairs = [(a, rows, 2) for a in range(3)]
    last = out_rows - 1
    acc1[last] += taps(x1, both, w1, near, pairs)
    right[last, :, pl.ds(0, cols), :] += as_frames(taps(x1, even, w1, far, pairs))

    def sums(parts, s, q, v):
        v8 = v.reshape(cols // 8, 8, c_out)
        return s + jnp.sum(v8, axis=0), q + jnp.sum(v8 * v8, axis=0)

    def stat_copy(phase, owner, peer, k):
        return pltpu.make_async_remote_copy(
            src_ref=stats.at[phase, me], dst_ref=stats.at[phase, owner],
            send_sem=stat_send.at[phase, k], recv_sem=stat_recv.at[phase, owner],
            device_id={"ha": peer}, device_id_type=MESH,
        )

    def send_stats(phase, s, q):
        stats[phase, me] = jnp.concatenate(
            [jnp.sum(s, axis=0, keepdims=True), jnp.sum(q, axis=0, keepdims=True)], axis=0
        )

        @pl.loop(1, n)
        def _(k):
            stat_copy(phase, me, lax.rem(me + k, n), k).start()

    per_group = c_out // GROUPS
    members = float(frames * out_rows * n * cols * per_group)

    def wait_stats(phase):
        @pl.loop(1, n)
        def _(k):
            peer = lax.rem(me + k, n)
            stat_copy(phase, peer, peer, k).wait_recv()

        both_sums = jnp.sum(stats[phase], axis=0)
        lane = lax.broadcasted_iota(jnp.int32, (8, c_out), 1)

        def grouped(v):
            v = jnp.broadcast_to(v, (8, c_out))
            step = 1
            while step < per_group:
                below = pltpu.roll(v, step, 1)
                above = pltpu.roll(v, c_out - step, 1)
                v = v + jnp.where((lane & step) == 0, above, below)
                step *= 2
            return v[0:1]

        center = grouped(both_sums[0:1]) / members
        spread = jnp.maximum(grouped(both_sums[1:2]) / members - center * center, 0.0)
        return center, lax.rsqrt(spread + 1e-06)

    def activate(v, center, scale, shift):
        v = (v - center) * scale + shift
        return (v / (1.0 + jnp.exp(-v))).astype(BF16)

    s = q = jnp.zeros((8, c_out), F32)
    for i in range(out_rows):
        for t in range(frames):
            span = pl.ds(t * cols, cols)
            v = acc1[i, span, :] + right[i, t, pl.ds(1, cols), :]
            acc1[i, span, :] = v
            s, q = sums(None, s, q, v)
    send_stats(0, s, q)

    for i in range(total + 3, len(copies)):
        copies[i].wait()

    center, inverse = wait_stats(0)
    scale = inverse * params[0]
    shift = params[1]
    for t in range(frames):
        for i in range(out_rows):
            v = activate(acc1[i, pl.ds(t * cols, cols), :], center, scale, shift)
            x2[1 + i, pl.ds((past + t) * cols, cols), :] = v
            if t >= frames - past:
                next_cache[t - frames + past, i] = v

        @pl.when(has_up)
        def _():
            hid_copy(True, past + t).start()

        @pl.when(has_down)
        def _():
            hid_copy(False, past + t).start()

    everything = slice(0, c_out)

    def mix(i, c, pairs):
        return taps(x2, everything, w2, pl.ds(c * c_out, c_out), pairs)

    for i in range(out_rows):
        pairs = [(a, i + b, b) for b in range(3) if 1 <= i + b <= out_rows for a in range(3)]
        left[i, :, pl.ds(8, cols), :] = as_frames(mix(i, 0, pairs))
        acc2[i] = mix(i, 1, pairs)
        right[i, :, pl.ds(0, cols), :] = as_frames(mix(i, 2, pairs))

    @pl.when(has_up)
    def _():
        for t in range(total):
            hid_copy(False, t).wait_recv()

    @pl.when(has_down)
    def _():
        for t in range(total):
            hid_copy(True, t).wait_recv()

    s = q = jnp.zeros((8, c_out), F32)
    for i in range(out_rows):
        pairs = [(a, i + b, b) for b in range(3) if not 1 <= i + b <= out_rows for a in range(3)]
        if pairs:
            left[i, :, pl.ds(8, cols), :] += as_frames(mix(i, 0, pairs))
            acc2[i] += mix(i, 1, pairs)
            right[i, :, pl.ds(0, cols), :] += as_frames(mix(i, 2, pairs))
        for t in range(frames):
            span = pl.ds(t * cols, cols)
            v = acc2[i, span, :] + left[i, t, pl.ds(7, cols), :] + right[i, t, pl.ds(1, cols), :]
            acc2[i, span, :] = v
            s, q = sums(None, s, q, v)
    send_stats(1, s, q)

    center, inverse = wait_stats(1)
    scale = inverse * params[2]
    shift = params[3]
    for t in range(frames):
        for i in range(out_rows):
            encoded[t, i] = activate(acc2[i, pl.ds(t * cols, cols), :], center, scale, shift)

    @pl.when(has_up)
    def _():
        for t in range(total):
            rim_copy(t).wait_send()
            hid_copy(True, t).wait_send()

    @pl.when(has_down)
    def _():
        for t in range(total):
            hid_copy(False, t).wait_send()

    for phase in range(2):

        @pl.loop(1, n)
        def _(k):
            stat_copy(phase, me, lax.rem(me + k, n), k).wait_send()


def local(n, video, cache_video, cache_hidden, kernel_down, gain_down, shift_down, kernel_mix, gain_mix, shift_mix):
    frames, rows, width, c_in = video.shape
    past, out_rows, cols, c_out = cache_hidden.shape
    total = frames + past
    hbm = pl.BlockSpec(memory_space=pltpu.HBM)
    vmem = pl.BlockSpec(memory_space=pltpu.VMEM)
    row = lambda v: v.reshape(1, c_out)
    return pl.pallas_call(
        functools.partial(kernel, n),
        out_shape=(
            jax.ShapeDtypeStruct((frames, out_rows, cols, c_out), BF16),
            jax.ShapeDtypeStruct((past, out_rows, cols, c_out), BF16),
        ),
        in_specs=[hbm] * 9,
        out_specs=(vmem, vmem),
        scratch_shapes=[
            pltpu.VMEM((total, rows, width, c_in), BF16),
            pltpu.VMEM((total, width, c_in), BF16),
            pltpu.VMEM((rows, width, c_in), F32),
            pltpu.VMEM((rows + 1, total * cols, 2 * c_in), BF16),
            pltpu.VMEM((9, 3 * c_in, c_out), BF16),
            pltpu.VMEM((9, 3 * c_out, c_out), BF16),
            pltpu.VMEM((out_rows + 2, total * cols, c_out), BF16),
            pltpu.VMEM((out_rows, frames * cols, c_out), F32),
            pltpu.VMEM((out_rows, frames * cols, c_out), F32),
            pltpu.VMEM((out_rows, frames, cols + 8, c_out), F32),
            pltpu.VMEM((out_rows, frames, cols + 8, c_out), F32),
            pltpu.VMEM((2, n, 2, c_out), F32),
            pltpu.VMEM((4, 1, c_out), F32),
            pltpu.SemaphoreType.DMA((total + 10 + past * out_rows,)),
            pltpu.SemaphoreType.DMA((total,)),
            pltpu.SemaphoreType.DMA((total,)),
            pltpu.SemaphoreType.DMA((2, total)),
            pltpu.SemaphoreType.DMA((2, total)),
            pltpu.SemaphoreType.DMA((2, n)),
            pltpu.SemaphoreType.DMA((2, n)),
        ],
        compiler_params=pltpu.CompilerParams(
            collective_id=0, has_side_effects=True, vmem_limit_bytes=67043328
        ),
    )(
        video,
        cache_video,
        cache_hidden,
        kernel_down.reshape(9, 3 * c_in, c_out),
        row(gain_down),
        row(shift_down),
        kernel_mix.reshape(9, 3 * c_out, c_out),
        row(gain_mix),
        row(shift_mix),
    )


def solution(mesh):
    split = P("groups", "ha", None, None)
    return jax.shard_map(
        functools.partial(local, mesh.shape["ha"]),
        mesh=mesh,
        in_specs=(split, split, split) + (P(),) * 6,
        out_specs=(split, split),
        check_vma=False,
    )
```

```python
import functools

import jax
import jax.numpy as jnp
from jax import lax
from jax.experimental import pallas as pl
from jax.experimental.pallas import tpu as pltpu
from jax.sharding import PartitionSpec as P

GROUPS = 32
MESH = pl.DeviceIdType.MESH
F32 = jnp.float32
BF16 = jnp.bfloat16


def kernel(
    n,
    video,
    cache_video,
    cache_hidden,
    w_down,
    gain_down,
    shift_down,
    w_mix,
    gain_mix,
    shift_mix,
    encoded,
    next_cache,
    vid,
    rim,
    raw,
    x1,
    w1,
    w2,
    x2,
    acc1,
    acc2,
    right,
    left,
    stats,
    params,
    sent,
    got,
    means,
    load_sem,
    rim_send,
    rim_recv,
    hid_send,
    hid_recv,
    stat_send,
    stat_recv,
):
    frames, rows, width, c_in = video.shape
    past = cache_video.shape[0]
    total = frames + past
    out_rows, cols, c_out = cache_hidden.shape[1:]
    m = frames * cols
    me = lax.axis_index("ha")
    has_up = me > 0
    has_down = me < n - 1

    barrier = pltpu.get_barrier_semaphore()

    @pl.loop(1, n)
    def _(k):
        pl.semaphore_signal(barrier, inc=1, device_id={"ha": lax.rem(me + k, n)}, device_id_type=MESH)

    loads = []
    for t in range(total):
        src = cache_video.at[t] if t < past else video.at[t - past]
        loads.append((src, vid.at[t]))
    for a in range(3):
        loads.append((w_down.at[pl.ds(3 * a, 3)], w1.at[pl.ds(3 * a, 3)]))
    for a in range(3):
        loads.append((w_mix.at[pl.ds(3 * a, 3)], w2.at[pl.ds(3 * a, 3)]))
    for t in range(past):
        for r in range(out_rows):
            loads.append((cache_hidden.at[t, r], x2.at[1 + r, pl.ds(t * cols, cols)]))
    for i, param in enumerate((gain_down, shift_down, gain_mix, shift_mix)):
        loads.append((param, params.at[i]))
    copies = [pltpu.make_async_copy(s, d, load_sem.at[i]) for i, (s, d) in enumerate(loads)]
    for copy in copies:
        copy.start()

    right[:, :, pl.ds(cols, 8), :] = jnp.zeros(right.shape[:2] + (8, c_out), F32)
    left[:, :, pl.ds(0, 8), :] = jnp.zeros(left.shape[:2] + (8, c_out), F32)

    def rim_copy(t):
        src = cache_video.at[t, 0] if t < past else video.at[t - past, 0]
        return pltpu.make_async_remote_copy(
            src_ref=src, dst_ref=rim.at[t], send_sem=rim_send.at[t], recv_sem=rim_recv.at[t],
            device_id={"ha": me - 1}, device_id_type=MESH,
        )

    def hid_copy(up, t):
        side = 0 if up else 1
        if t < past:
            src = cache_hidden.at[t, 0 if up else out_rows - 1]
            dst = x2.at[out_rows + 1 if up else 0, pl.ds(t * cols, cols)]
        elif t < total:
            src, dst = sent.at[side, t - past], got.at[side, t - past]
        else:
            src, dst = means.at[side], means.at[2 + side]
        return pltpu.make_async_remote_copy(
            src_ref=src, dst_ref=dst,
            send_sem=hid_send.at[side, t], recv_sem=hid_recv.at[side, t],
            device_id={"ha": me - 1 if up else me + 1}, device_id_type=MESH,
        )

    pl.semaphore_wait(barrier, n - 1)

    @pl.when(has_up)
    def _():
        for t in range(total):
            rim_copy(t).start()
        for t in range(past):
            hid_copy(True, t).start()

    @pl.when(has_down)
    def _():
        for t in range(past):
            hid_copy(False, t).start()

    @pl.when(jnp.logical_not(has_up))
    def _():
        x2[0] = jnp.zeros(x2.shape[1:], BF16)

    @pl.when(jnp.logical_not(has_down))
    def _():
        x2[out_rows + 1] = jnp.zeros(x2.shape[1:], BF16)
        x1[rows] = jnp.zeros(x1.shape[1:], BF16)

    def split(src, slot, r, t):
        raw[slot] = src.astype(F32)
        x1[r, pl.ds(t * cols, cols), 0:c_in] = raw[slot, pl.ds(0, cols, stride=2), :].astype(BF16)
        x1[r, pl.ds(t * cols, cols), c_in:] = raw[slot, pl.ds(1, cols, stride=2), :].astype(BF16)

    for t in range(total):
        copies[t].wait()
        for r in range(rows):
            split(vid[t, r], r, r, t)
    for a in range(3):
        copies[total + a].wait()

    def taps(x, lanes, w, depth, pairs):
        lhs = jnp.concatenate([x[r, pl.ds(a * cols, m), lanes] for a, r, b in pairs], axis=1)
        rhs = jnp.concatenate([w[3 * a + b, depth, :] for a, r, b in pairs], axis=0)
        return jnp.dot(lhs, rhs, preferred_element_type=F32)

    both, even = slice(0, 2 * c_in), slice(0, c_in)
    near, far = slice(0, 2 * c_in), slice(2 * c_in, 3 * c_in)

    def as_frames(v):
        return v.reshape(frames, cols, c_out)

    def sums(s, q, v):
        v8 = v.reshape(cols // 8, 8, c_out)
        return s + jnp.sum(v8, axis=0), q + jnp.sum(v8 * v8, axis=0)

    def stat_copy(phase, owner, peer, k):
        return pltpu.make_async_remote_copy(
            src_ref=stats.at[phase, me], dst_ref=stats.at[phase, owner],
            send_sem=stat_send.at[phase, k], recv_sem=stat_recv.at[phase, owner],
            device_id={"ha": peer}, device_id_type=MESH,
        )

    def send_stats(phase, s, q):
        stats[phase, me] = jnp.concatenate(
            [jnp.sum(s, axis=0, keepdims=True), jnp.sum(q, axis=0, keepdims=True)], axis=0
        )

        @pl.loop(1, n)
        def _(k):
            stat_copy(phase, me, lax.rem(me + k, n), k).start()

    per_group = c_out // GROUPS
    members = float(frames * out_rows * n * cols * per_group)

    def wait_stats(phase):
        @pl.loop(1, n)
        def _(k):
            peer = lax.rem(me + k, n)
            stat_copy(phase, peer, peer, k).wait_recv()

        both_sums = jnp.sum(stats[phase], axis=0)
        lane = lax.broadcasted_iota(jnp.int32, (8, c_out), 1)

        def grouped(v):
            v = jnp.broadcast_to(v, (8, c_out))
            step = 1
            while step < per_group:
                below = pltpu.roll(v, step, 1)
                above = pltpu.roll(v, c_out - step, 1)
                v = v + jnp.where((lane & step) == 0, above, below)
                step *= 2
            return v[0:1]

        center = grouped(both_sums[0:1]) / members
        spread = jnp.maximum(grouped(both_sums[1:2]) / members - center * center, 0.0)
        return center, lax.rsqrt(spread + 1e-06)

    def activate(v, center, scale, shift):
        v = (v - center) * scale + shift
        return (v / (1.0 + jnp.exp(-v))).astype(BF16)

    def down_row(i):
        pairs = [(a, 2 * i + b, b) for b in range(3) if 2 * i + b < rows for a in range(3)]
        acc1[i] = taps(x1, both, w1, near, pairs)
        right[i, :, pl.ds(0, cols), :] = as_frames(taps(x1, even, w1, far, pairs))

    def shifted_row(i, s, q):
        row = jnp.zeros((8, c_out), F32)
        for t in range(frames):
            span = pl.ds(t * cols, cols)
            v = acc1[i, span, :] + right[i, t, pl.ds(1, cols), :]
            acc1[i, span, :] = v
            row, q = sums(row, q, v)
        return s + row, q, jnp.sum(row, axis=0, keepdims=True) / float(m)

    def centre_row(side, i, mean):
        means[side] = mean
        for t in range(frames):
            sent[side, t] = (acc1[i, pl.ds(t * cols, cols), :] - mean).astype(BF16)

    s = q = jnp.zeros((8, c_out), F32)
    last = out_rows - 1
    for i in range(last):
        down_row(i)
        s, q, mean = shifted_row(i, s, q)
        if i == 0:
            centre_row(0, i, mean)

            @pl.when(has_up)
            def _():
                for t in range(past, total + 1):
                    hid_copy(True, t).start()

    down_row(last)

    @pl.when(has_down)
    def _():
        for t in range(total):
            rim_copy(t).wait_recv()
            split(rim[t], t % rows, rows, t)

    pairs = [(a, rows, 2) for a in range(3)]
    acc1[last] += taps(x1, both, w1, near, pairs)
    right[last, :, pl.ds(0, cols), :] += as_frames(taps(x1, even, w1, far, pairs))
    s, q, mean = shifted_row(last, s, q)
    send_stats(0, s, q)
    centre_row(1, last, mean)

    @pl.when(has_down)
    def _():
        for t in range(past, total + 1):
            hid_copy(False, t).start()

    for i in range(total + 3, len(copies)):
        copies[i].wait()

    everything = slice(0, c_out)

    def mix(i, c, pairs):
        return taps(x2, everything, w2, pl.ds(c * c_out, c_out), pairs)

    center, inverse = wait_stats(0)
    scale = inverse * params[0]
    shift = params[1]
    for t in range(frames):
        for i in range(out_rows):
            v = activate(acc1[i, pl.ds(t * cols, cols), :], center, scale, shift)
            x2[1 + i, pl.ds((past + t) * cols, cols), :] = v
            if t >= frames - past:
                next_cache[t - frames + past, i] = v

    for i in range(out_rows):
        pairs = [(a, i + b, b) for b in range(3) if 1 <= i + b <= out_rows for a in range(3)]
        left[i, :, pl.ds(8, cols), :] = as_frames(mix(i, 0, pairs))
        acc2[i] = mix(i, 1, pairs)
        right[i, :, pl.ds(0, cols), :] = as_frames(mix(i, 2, pairs))

    def receive(up):
        side = 0 if up else 1
        for t in range(total + 1):
            hid_copy(up, t).wait_recv()
        offset = center - means[2 + side]
        for t in range(frames):
            x2[out_rows + 1 if up else 0, pl.ds((past + t) * cols, cols), :] = activate(
                got[side, t].astype(F32), offset, scale, shift
            )

    @pl.when(has_up)
    def _():
        receive(False)

    @pl.when(has_down)
    def _():
        receive(True)

    s = q = jnp.zeros((8, c_out), F32)
    for i in range(out_rows):
        pairs = [(a, i + b, b) for b in range(3) if not 1 <= i + b <= out_rows for a in range(3)]
        if pairs:
            left[i, :, pl.ds(8, cols), :] += as_frames(mix(i, 0, pairs))
            acc2[i] += mix(i, 1, pairs)
            right[i, :, pl.ds(0, cols), :] += as_frames(mix(i, 2, pairs))
        for t in range(frames):
            span = pl.ds(t * cols, cols)
            v = acc2[i, span, :] + left[i, t, pl.ds(7, cols), :] + right[i, t, pl.ds(1, cols), :]
            acc2[i, span, :] = v
            s, q = sums(s, q, v)
    send_stats(1, s, q)

    center, inverse = wait_stats(1)
    scale = inverse * params[2]
    shift = params[3]
    for t in range(frames):
        for i in range(out_rows):
            encoded[t, i] = activate(acc2[i, pl.ds(t * cols, cols), :], center, scale, shift)

    @pl.when(has_up)
    def _():
        for t in range(total):
            rim_copy(t).wait_send()
        for t in range(total + 1):
            hid_copy(True, t).wait_send()

    @pl.when(has_down)
    def _():
        for t in range(total + 1):
            hid_copy(False, t).wait_send()

    for phase in range(2):

        @pl.loop(1, n)
        def _(k):
            stat_copy(phase, me, lax.rem(me + k, n), k).wait_send()


def local(n, video, cache_video, cache_hidden, kernel_down, gain_down, shift_down, kernel_mix, gain_mix, shift_mix):
    frames, rows, width, c_in = video.shape
    past, out_rows, cols, c_out = cache_hidden.shape
    total = frames + past
    hbm = pl.BlockSpec(memory_space=pltpu.HBM)
    vmem = pl.BlockSpec(memory_space=pltpu.VMEM)
    row = lambda v: v.reshape(1, c_out)
    return pl.pallas_call(
        functools.partial(kernel, n),
        out_shape=(
            jax.ShapeDtypeStruct((frames, out_rows, cols, c_out), BF16),
            jax.ShapeDtypeStruct((past, out_rows, cols, c_out), BF16),
        ),
        in_specs=[hbm] * 9,
        out_specs=(vmem, vmem),
        scratch_shapes=[
            pltpu.VMEM((total, rows, width, c_in), BF16),
            pltpu.VMEM((total, width, c_in), BF16),
            pltpu.VMEM((rows, width, c_in), F32),
            pltpu.VMEM((rows + 1, total * cols, 2 * c_in), BF16),
            pltpu.VMEM((9, 3 * c_in, c_out), BF16),
            pltpu.VMEM((9, 3 * c_out, c_out), BF16),
            pltpu.VMEM((out_rows + 2, total * cols, c_out), BF16),
            pltpu.VMEM((out_rows, frames * cols, c_out), F32),
            pltpu.VMEM((out_rows, frames * cols, c_out), F32),
            pltpu.VMEM((out_rows, frames, cols + 8, c_out), F32),
            pltpu.VMEM((out_rows, frames, cols + 8, c_out), F32),
            pltpu.VMEM((2, n, 2, c_out), F32),
            pltpu.VMEM((4, 1, c_out), F32),
            pltpu.VMEM((2, frames, cols, c_out), BF16),
            pltpu.VMEM((2, frames, cols, c_out), BF16),
            pltpu.VMEM((4, 1, c_out), F32),
            pltpu.SemaphoreType.DMA((total + 10 + past * out_rows,)),
            pltpu.SemaphoreType.DMA((total,)),
            pltpu.SemaphoreType.DMA((total,)),
            pltpu.SemaphoreType.DMA((2, total + 1)),
            pltpu.SemaphoreType.DMA((2, total + 1)),
            pltpu.SemaphoreType.DMA((2, n)),
            pltpu.SemaphoreType.DMA((2, n)),
        ],
        compiler_params=pltpu.CompilerParams(
            collective_id=0, has_side_effects=True, vmem_limit_bytes=67043328
        ),
    )(
        video,
        cache_video,
        cache_hidden,
        kernel_down.reshape(9, 3 * c_in, c_out),
        row(gain_down),
        row(shift_down),
        kernel_mix.reshape(9, 3 * c_out, c_out),
        row(gain_mix),
        row(shift_mix),
    )


def solution(mesh):
    split = P("groups", "ha", None, None)
    return jax.shard_map(
        functools.partial(local, mesh.shape["ha"]),
        mesh=mesh,
        in_specs=(split, split, split) + (P(),) * 6,
        out_specs=(split, split),
        check_vma=False,
    )
```

```python
import functools

import jax
import jax.numpy as jnp
from jax import lax
from jax.experimental import pallas as pl
from jax.experimental.pallas import tpu as pltpu
from jax.sharding import PartitionSpec as P

GROUPS = 32
MESH = pl.DeviceIdType.MESH
F32 = jnp.float32
BF16 = jnp.bfloat16


def kernel(
    n,
    video,
    cache_video,
    cache_hidden,
    w_down,
    gain_down,
    shift_down,
    w_mix,
    gain_mix,
    shift_mix,
    encoded,
    next_cache,
    vid,
    rim,
    raw,
    x1,
    w1,
    w2,
    x2,
    acc1,
    acc2,
    right,
    left,
    stats,
    params,
    sent,
    got,
    means,
    load_sem,
    rim_send,
    rim_recv,
    hid_send,
    hid_recv,
    stat_send,
    stat_recv,
):
    frames, rows, width, c_in = video.shape
    past = cache_video.shape[0]
    total = frames + past
    out_rows, cols, c_out = cache_hidden.shape[1:]
    m = frames * cols
    me = lax.axis_index("ha")
    has_up = me > 0
    has_down = me < n - 1

    barrier = pltpu.get_barrier_semaphore()

    @pl.loop(1, n)
    def _(k):
        pl.semaphore_signal(barrier, inc=1, device_id={"ha": lax.rem(me + k, n)}, device_id_type=MESH)

    loads = []
    for t in range(total):
        src = cache_video.at[t] if t < past else video.at[t - past]
        loads.append((src, vid.at[t]))
    for a in range(3):
        loads.append((w_down.at[pl.ds(3 * a, 3)], w1.at[pl.ds(3 * a, 3)]))
    for a in range(3):
        loads.append((w_mix.at[pl.ds(3 * a, 3)], w2.at[pl.ds(3 * a, 3)]))
    for t in range(past):
        for r in range(out_rows):
            loads.append((cache_hidden.at[t, r], x2.at[1 + r, pl.ds(t * cols, cols)]))
    for i, param in enumerate((gain_down, shift_down, gain_mix, shift_mix)):
        loads.append((param, params.at[i]))
    copies = [pltpu.make_async_copy(s, d, load_sem.at[i]) for i, (s, d) in enumerate(loads)]
    for copy in copies:
        copy.start()

    right[:, :, pl.ds(cols, 8), :] = jnp.zeros(right.shape[:2] + (8, c_out), F32)
    left[:, :, pl.ds(0, 8), :] = jnp.zeros(left.shape[:2] + (8, c_out), F32)

    def rim_copy(t):
        src = cache_video.at[t, 0] if t < past else video.at[t - past, 0]
        return pltpu.make_async_remote_copy(
            src_ref=src, dst_ref=rim.at[t], send_sem=rim_send.at[t], recv_sem=rim_recv.at[t],
            device_id={"ha": me - 1}, device_id_type=MESH,
        )

    def hid_copy(up, t):
        side = 0 if up else 1
        if t < past:
            src = cache_hidden.at[t, 0 if up else out_rows - 1]
            dst = x2.at[out_rows + 1 if up else 0, pl.ds(t * cols, cols)]
        elif t < total:
            src, dst = sent.at[side, t - past], got.at[side, t - past]
        else:
            src, dst = means.at[side], means.at[2 + side]
        return pltpu.make_async_remote_copy(
            src_ref=src, dst_ref=dst,
            send_sem=hid_send.at[side, t], recv_sem=hid_recv.at[side, t],
            device_id={"ha": me - 1 if up else me + 1}, device_id_type=MESH,
        )

    pl.semaphore_wait(barrier, n - 1)

    @pl.when(has_up)
    def _():
        for t in range(total):
            rim_copy(t).start()
        for t in range(past):
            hid_copy(True, t).start()

    @pl.when(has_down)
    def _():
        for t in range(past):
            hid_copy(False, t).start()

    @pl.when(jnp.logical_not(has_up))
    def _():
        x2[0] = jnp.zeros(x2.shape[1:], BF16)

    @pl.when(jnp.logical_not(has_down))
    def _():
        x2[out_rows + 1] = jnp.zeros(x2.shape[1:], BF16)
        x1[rows] = jnp.zeros(x1.shape[1:], BF16)

    def split(src, slot, r, t):
        raw[slot] = src.astype(F32)
        x1[r, pl.ds(t * cols, cols), 0:c_in] = raw[slot, pl.ds(0, cols, stride=2), :].astype(BF16)
        x1[r, pl.ds(t * cols, cols), c_in:] = raw[slot, pl.ds(1, cols, stride=2), :].astype(BF16)

    for t in range(total):
        copies[t].wait()
        for r in range(rows):
            split(vid[t, r], r, r, t)
    for a in range(3):
        copies[total + a].wait()

    def taps(x, lanes, w, depth, pairs):
        lhs = jnp.concatenate([x[r, pl.ds(a * cols, m), lanes] for a, r, b in pairs], axis=1)
        rhs = jnp.concatenate([w[3 * a + b, depth, :] for a, r, b in pairs], axis=0)
        return jnp.dot(lhs, rhs, preferred_element_type=F32)

    both, even = slice(0, 2 * c_in), slice(0, c_in)
    near, far = slice(0, 2 * c_in), slice(2 * c_in, 3 * c_in)

    def as_frames(v):
        return v.reshape(frames, cols, c_out)

    def sums(s, q, v):
        v8 = v.reshape(cols // 8, 8, c_out)
        return s + jnp.sum(v8, axis=0), q + jnp.sum(v8 * v8, axis=0)

    def stat_copy(phase, owner, peer, k):
        return pltpu.make_async_remote_copy(
            src_ref=stats.at[phase, me], dst_ref=stats.at[phase, owner],
            send_sem=stat_send.at[phase, k], recv_sem=stat_recv.at[phase, owner],
            device_id={"ha": peer}, device_id_type=MESH,
        )

    def send_stats(phase, s, q):
        stats[phase, me] = jnp.concatenate(
            [jnp.sum(s, axis=0, keepdims=True), jnp.sum(q, axis=0, keepdims=True)], axis=0
        )

        @pl.loop(1, n)
        def _(k):
            stat_copy(phase, me, lax.rem(me + k, n), k).start()

    per_group = c_out // GROUPS
    members = float(frames * out_rows * n * cols * per_group)

    def wait_stats(phase):
        @pl.loop(1, n)
        def _(k):
            peer = lax.rem(me + k, n)
            stat_copy(phase, peer, peer, k).wait_recv()

        both_sums = jnp.sum(stats[phase], axis=0)
        lane = lax.broadcasted_iota(jnp.int32, (8, c_out), 1)

        def grouped(v):
            v = jnp.broadcast_to(v, (8, c_out))
            step = 1
            while step < per_group:
                below = pltpu.roll(v, step, 1)
                above = pltpu.roll(v, c_out - step, 1)
                v = v + jnp.where((lane & step) == 0, above, below)
                step *= 2
            return v[0:1]

        center = grouped(both_sums[0:1]) / members
        spread = jnp.maximum(grouped(both_sums[1:2]) / members - center * center, 0.0)
        return center, lax.rsqrt(spread + 1e-06)

    def activate(v, center, scale, shift):
        v = (v - center) * scale + shift
        return (v / (1.0 + jnp.exp(-v))).astype(BF16)

    def down_row(i):
        pairs = [(a, 2 * i + b, b) for b in range(3) if 2 * i + b < rows for a in range(3)]
        acc1[i] = taps(x1, both, w1, near, pairs)
        right[i, :, pl.ds(0, cols), :] = as_frames(taps(x1, even, w1, far, pairs))

    def shifted_row(i, s, q):
        row = jnp.zeros((8, c_out), F32)
        for t in range(frames):
            span = pl.ds(t * cols, cols)
            v = acc1[i, span, :] + right[i, t, pl.ds(1, cols), :]
            acc1[i, span, :] = v
            row, q = sums(row, q, v)
        return s + row, q, jnp.sum(row, axis=0, keepdims=True) / float(m)

    def centre_row(side, i, mean):
        means[side] = mean
        for t in range(frames):
            sent[side, t] = (acc1[i, pl.ds(t * cols, cols), :] - mean).astype(BF16)

    s = q = jnp.zeros((8, c_out), F32)
    last = out_rows - 1
    for i in range(last):
        down_row(i)
        s, q, mean = shifted_row(i, s, q)
        if i == 0:
            centre_row(0, i, mean)

            @pl.when(has_up)
            def _():
                for t in range(past, total + 1):
                    hid_copy(True, t).start()

    down_row(last)

    @pl.when(has_down)
    def _():
        for t in range(total):
            rim_copy(t).wait_recv()
            split(rim[t], t % rows, rows, t)

    pairs = [(a, rows, 2) for a in range(3)]
    acc1[last] += taps(x1, both, w1, near, pairs)
    right[last, :, pl.ds(0, cols), :] += as_frames(taps(x1, even, w1, far, pairs))
    s, q, mean = shifted_row(last, s, q)
    send_stats(0, s, q)
    centre_row(1, last, mean)

    @pl.when(has_down)
    def _():
        for t in range(past, total + 1):
            hid_copy(False, t).start()

    for i in range(total + 3, len(copies)):
        copies[i].wait()

    everything = slice(0, c_out)

    def mix(i, c, pairs):
        return taps(x2, everything, w2, pl.ds(c * c_out, c_out), pairs)

    center, inverse = wait_stats(0)
    scale = inverse * params[0]
    shift = params[1]
    for t in range(frames):
        for i in range(out_rows):
            v = activate(acc1[i, pl.ds(t * cols, cols), :], center, scale, shift)
            x2[1 + i, pl.ds((past + t) * cols, cols), :] = v
            if t >= frames - past:
                next_cache[t - frames + past, i] = v

    for i in range(out_rows):
        pairs = [(a, i + b, b) for b in range(3) if 1 <= i + b <= out_rows for a in range(3)]
        left[i, :, pl.ds(8, cols), :] = as_frames(mix(i, 0, pairs))
        acc2[i] = mix(i, 1, pairs)
        right[i, :, pl.ds(0, cols), :] = as_frames(mix(i, 2, pairs))

    def receive(up):
        side = 0 if up else 1
        for t in range(total + 1):
            hid_copy(up, t).wait_recv()
        offset = center - means[2 + side]
        for t in range(frames):
            x2[out_rows + 1 if up else 0, pl.ds((past + t) * cols, cols), :] = activate(
                got[side, t].astype(F32), offset, scale, shift
            )

    @pl.when(has_up)
    def _():
        receive(False)

    @pl.when(has_down)
    def _():
        receive(True)

    s = q = jnp.zeros((8, c_out), F32)
    for i in range(out_rows):
        pairs = [(a, i + b, b) for b in range(3) if not 1 <= i + b <= out_rows for a in range(3)]
        if pairs:
            left[i, :, pl.ds(8, cols), :] += as_frames(mix(i, 0, pairs))
            acc2[i] += mix(i, 1, pairs)
            right[i, :, pl.ds(0, cols), :] += as_frames(mix(i, 2, pairs))
        for t in range(frames):
            span = pl.ds(t * cols, cols)
            v = acc2[i, span, :] + left[i, t, pl.ds(7, cols), :] + right[i, t, pl.ds(1, cols), :]
            acc2[i, span, :] = v
            s, q = sums(s, q, v)
    send_stats(1, s, q)

    center, inverse = wait_stats(1)
    scale = inverse * params[2]
    shift = params[3]
    for t in range(frames):
        for i in range(out_rows):
            encoded[t, i] = activate(acc2[i, pl.ds(t * cols, cols), :], center, scale, shift)

    @pl.when(has_up)
    def _():
        for t in range(total):
            rim_copy(t).wait_send()
        for t in range(total + 1):
            hid_copy(True, t).wait_send()

    @pl.when(has_down)
    def _():
        for t in range(total + 1):
            hid_copy(False, t).wait_send()

    for phase in range(2):

        @pl.loop(1, n)
        def _(k):
            stat_copy(phase, me, lax.rem(me + k, n), k).wait_send()


def local(n, video, cache_video, cache_hidden, kernel_down, gain_down, shift_down, kernel_mix, gain_mix, shift_mix):
    frames, rows, width, c_in = video.shape
    past, out_rows, cols, c_out = cache_hidden.shape
    total = frames + past
    hbm = pl.BlockSpec(memory_space=pltpu.HBM)
    vmem = pl.BlockSpec(memory_space=pltpu.VMEM)
    row = lambda v: v.reshape(1, c_out)
    return pl.pallas_call(
        functools.partial(kernel, n),
        out_shape=(
            jax.ShapeDtypeStruct((frames, out_rows, cols, c_out), BF16),
            jax.ShapeDtypeStruct((past, out_rows, cols, c_out), BF16),
        ),
        in_specs=[hbm] * 9,
        out_specs=(vmem, vmem),
        scratch_shapes=[
            pltpu.VMEM((total, rows, width, c_in), BF16),
            pltpu.VMEM((total, width, c_in), BF16),
            pltpu.VMEM((rows, width, c_in), F32),
            pltpu.VMEM((rows + 1, total * cols, 2 * c_in), BF16),
            pltpu.VMEM((9, 3 * c_in, c_out), BF16),
            pltpu.VMEM((9, 3 * c_out, c_out), BF16),
            pltpu.VMEM((out_rows + 2, total * cols, c_out), BF16),
            pltpu.VMEM((out_rows, frames * cols, c_out), F32),
            pltpu.VMEM((out_rows, frames * cols, c_out), F32),
            pltpu.VMEM((out_rows, frames, cols + 8, c_out), F32),
            pltpu.VMEM((out_rows, frames, cols + 8, c_out), F32),
            pltpu.VMEM((2, n, 2, c_out), F32),
            pltpu.VMEM((4, 1, c_out), F32),
            pltpu.VMEM((2, frames, cols, c_out), BF16),
            pltpu.VMEM((2, frames, cols, c_out), BF16),
            pltpu.VMEM((4, 1, c_out), F32),
            pltpu.SemaphoreType.DMA((total + 10 + past * out_rows,)),
            pltpu.SemaphoreType.DMA((total,)),
            pltpu.SemaphoreType.DMA((total,)),
            pltpu.SemaphoreType.DMA((2, total + 1)),
            pltpu.SemaphoreType.DMA((2, total + 1)),
            pltpu.SemaphoreType.DMA((2, n)),
            pltpu.SemaphoreType.DMA((2, n)),
        ],
        compiler_params=pltpu.CompilerParams(
            collective_id=0, has_side_effects=True, vmem_limit_bytes=48 * 1024 * 1024
        ),
    )(
        *(
            pltpu.with_memory_space_constraint(v, pltpu.HBM)
            for v in (
                video,
                cache_video,
                cache_hidden,
                kernel_down.reshape(9, 3 * c_in, c_out),
                row(gain_down),
                row(shift_down),
                kernel_mix.reshape(9, 3 * c_out, c_out),
                row(gain_mix),
                row(shift_mix),
            )
        )
    )


def solution(mesh):
    split = P("groups", "ha", None, None)
    return jax.shard_map(
        functools.partial(local, mesh.shape["ha"]),
        mesh=mesh,
        in_specs=(split, split, split) + (P(),) * 6,
        out_specs=(split, split),
        check_vma=False,
    )
```
